32 devices in a mesh: gx: 8 (over z, y), gy: 4 (over x, core).
Axes of the slice: x: 2, y: 2, z: 4, core: 2. Of those that a mesh axis runs over, the one named last changes fastest.
Arguments:
- prev_voltage: float32 [32, 32, 128, 128], P('gx', 'gy'), may hold values from -6 to 6
- source: float32 [32, 32, 128, 128], P('gx', 'gy'), may hold values from -30 to 30
- cap_over_h: float32 [32, 32, 128], P('gx', 'gy'), may hold values from 0.05 to 0.5
- diag_blocks: float32 [32, 32, 128, 128], P('gx', 'gy'), as said below
- inverse_blocks: float32 [32, 32, 128, 128], P('gx', 'gy'), as said below
- east_coupling: float32 [32, 32, 128, 128], P('gx', 'gy'), may hold values from 0 to 0.015625, as said below
- south_coupling: float32 [32, 32, 128, 128], P('gx', 'gy'), may hold values from 0 to 0.015625, as said below
- via_mask: int32 [32, 32, 2], P('gx', 'gy'), may hold values from 0 to 1, as said below
Outputs:
- voltage: float32 [32, 32, 128, 128], P('gx', 'gy')
- residual: float32 [32, 32, 128, 128], P('gx', 'gy')
The draws below stay inside these ranges and needn't reach their ends.
Inputs may be any that keep to these rules, and one draw needn't show every extreme that they name: `via_mask`: 1 where the via coupling to the east (index 0) or south (index 1) neighbour block is present. `east_coupling`: nonnegative; zero in the last block column, which has no east neighbour. `south_coupling`: nonnegative; zero in the last block row, which has no south neighbour. `diag_blocks`: symmetric; off the diagonal nonpositive; each diagonal entry is cap_over_h plus the sum of the magnitudes of all other entries in its row of the system matrix, live couplings included. `inverse_blocks`: the inverse of the matching block of diag_blocks, in float32.
All inputs are finite; a program needn't handle non-finite values.
Results may differ from the reference program's by a relative error of at most 0.0003.
Values sent between devices are 32-bit elements; how exact they have to be, the bound alone decides.
A program may use at most 128 MiB of HBM per device.

```python
import math
import jax
import jax.numpy as jnp
from jax import lax

BS = 128
SCEN = 128
ITERS = 4
BROWS = 32
BCOLS = 32


def grid_system(key):
    base = jax.random.fold_in(key, 11)
    keys = jax.random.split(base, 5)
    shape_four = (BROWS, BCOLS, BS, BS)
    inner_raw = jax.random.uniform(keys[0], shape_four, jnp.float32, 0.0, 2.0 / BS)
    inner_sym = 0.5 * (inner_raw + jnp.swapaxes(inner_raw, 2, 3))
    identity = jnp.eye(BS, dtype=jnp.float32)
    inner_off = inner_sym * (1.0 - identity)
    links = (jax.random.randint(keys[1], (BROWS, BCOLS, 2), 0, 4) < 3).astype(jnp.int32)
    col_live = (jnp.arange(BCOLS) < BCOLS - 1).astype(jnp.float32)[None, :, None, None]
    row_live = (jnp.arange(BROWS) < BROWS - 1).astype(jnp.float32)[:, None, None, None]
    east = jax.random.uniform(keys[2], shape_four, jnp.float32, 0.0, 2.0 / BS) * col_live
    south = jax.random.uniform(keys[3], shape_four, jnp.float32, 0.0, 2.0 / BS) * row_live
    capacity = jnp.exp(jax.random.uniform(keys[4], (BROWS, BCOLS, BS), jnp.float32, math.log(0.05), math.log(0.5)))
    link_float = links.astype(jnp.float32)
    east_live = east * link_float[:, :, 0][:, :, None, None]
    south_live = south * link_float[:, :, 1][:, :, None, None]
    row_total = jnp.sum(inner_off, axis=3) + jnp.sum(east_live, axis=3) + jnp.sum(south_live, axis=3)
    from_west = jnp.sum(east_live, axis=2)
    from_north = jnp.sum(south_live, axis=2)
    west_in = jnp.concatenate([jnp.zeros_like(from_west[:, :1]), from_west[:, :-1]], axis=1)
    north_in = jnp.concatenate([jnp.zeros_like(from_north[:1]), from_north[:-1]], axis=0)
    diagonal = row_total + west_in + north_in + capacity
    block = diagonal[..., None] * identity - inner_off
    inverse = jnp.linalg.inv(block).astype(jnp.float32)
    return (block, inverse, capacity, east, south, links)


def draw_diag_blocks(key, part):
    return grid_system(key)[0]


def draw_inverse_blocks(key, part):
    return grid_system(key)[1]


def draw_cap_over_h(key, part):
    return grid_system(key)[2]


def draw_east_coupling(key, part):
    return grid_system(key)[3]


def draw_south_coupling(key, part):
    return grid_system(key)[4]


def draw_via_mask(key, part):
    return grid_system(key)[5]


def draw_source(key, part):
    shape_four = (BROWS, BCOLS, BS, SCEN)
    row_frac = jnp.arange(BROWS, dtype=jnp.float32) / max(BROWS - 1, 1)
    col_frac = jnp.arange(BCOLS, dtype=jnp.float32) / max(BCOLS - 1, 1)
    scale = 0.5 * (1.0 + 2.0 * row_frac)[:, None, None, None] * (1.0 + 2.0 * col_frac)[None, :, None, None]
    rough = jax.random.truncated_normal(key, -6.0, 6.0, shape_four, jnp.float32)
    return (scale * rough).astype(jnp.float32)


def shard_levels(own_key, extent, cuts, least, largest):
    gain = 1.0
    for axis_at, blocks in cuts:
        draws = jax.random.uniform(jax.random.fold_in(jax.random.fold_in(own_key, 6), axis_at), (blocks,), jnp.float32, least / len(cuts), largest / len(cuts))
        gain = gain * jnp.repeat(jnp.exp(draws), extent[axis_at] // blocks).reshape((-1,) + (1,) * (len(extent) - 1 - axis_at))
    return gain


def centred(stream_key, dims, width, limit, cuts=(), held_as=jnp.bfloat16):
    values = jax.random.normal(stream_key, dims, jnp.float32) * width
    if len(cuts) > 0:
        values = shard_levels(stream_key, dims, cuts, -0.22, 0.18) * values
    return jnp.clip(values, min=-limit, max=limit).astype(held_as)


def setup_inputs(seed: int = 0) -> dict:
    splits = jax.random.split(jax.random.key(seed), 9)
    return {
        "prev_voltage": centred(splits[0], (BROWS, BCOLS, BS, SCEN), 1.0, 6.0, ((0, 8), (1, 4)), jnp.float32),
        "source": draw_source(jax.random.fold_in(splits[8], 71), 0),
        "cap_over_h": draw_cap_over_h(jax.random.fold_in(splits[8], 71), 0),
        "diag_blocks": draw_diag_blocks(jax.random.fold_in(splits[8], 71), 0),
        "inverse_blocks": draw_inverse_blocks(jax.random.fold_in(splits[8], 71), 0),
        "east_coupling": draw_east_coupling(jax.random.fold_in(splits[8], 71), 0),
        "south_coupling": draw_south_coupling(jax.random.fold_in(splits[8], 71), 0),
        "via_mask": draw_via_mask(jax.random.fold_in(splits[8], 71), 0),
    }


def blocks_times(blocks, values):
    return jnp.einsum('rcij,rcjs->rcis', blocks, values, precision=lax.Precision.HIGHEST)

def blocks_trans(blocks, values):
    return jnp.einsum('rcji,rcjs->rcis', blocks, values, precision=lax.Precision.HIGHEST)

def inner_prod(former, latter):
    return jnp.sum(former * latter, axis=(0, 1, 2))

def apply_matrix(values, diag_blocks, east_live, south_live):
    east_near = jnp.concatenate([values[:, 1:], jnp.zeros_like(values[:, :1])], axis=1)
    south_near = jnp.concatenate([values[1:], jnp.zeros_like(values[:1])], axis=0)
    across = blocks_trans(east_live, values)
    downward = blocks_trans(south_live, values)
    result = blocks_times(diag_blocks, values)
    result = result - blocks_times(east_live, east_near) - blocks_times(south_live, south_near)
    result = result - jnp.concatenate([jnp.zeros_like(across[:, :1]), across[:, :-1]], axis=1)
    result = result - jnp.concatenate([jnp.zeros_like(downward[:1]), downward[:-1]], axis=0)
    return result

def reference(prev_voltage, source, cap_over_h, diag_blocks, inverse_blocks, east_coupling, south_coupling, via_mask):
    links = via_mask.astype(east_coupling.dtype)
    east_live = east_coupling * links[:, :, 0][:, :, None, None]
    south_live = south_coupling * links[:, :, 1][:, :, None, None]
    load = cap_over_h[..., None] * prev_voltage + source
    voltage = prev_voltage
    residual = load - apply_matrix(voltage, diag_blocks, east_live, south_live)
    search = blocks_times(inverse_blocks, residual)
    direction = search
    gamma_now = inner_prod(residual, search)
    for iteration in range(ITERS):
        image = apply_matrix(direction, diag_blocks, east_live, south_live)
        step_size = gamma_now / inner_prod(direction, image)
        voltage = voltage + step_size * direction
        residual = residual - step_size * image
        if iteration + 1 < ITERS:
            search = blocks_times(inverse_blocks, residual)
            gamma_next = inner_prod(residual, search)
            direction = search + gamma_next / gamma_now * direction
            gamma_now = gamma_next
    return (voltage, residual)
```

```python
import functools

import jax
import jax.numpy as jnp
from jax import lax
from jax.experimental import pallas as pl
from jax.experimental.pallas import tpu as pltpu
from jax.sharding import PartitionSpec as P

ITERS = 4
STEPS = ITERS + 1
MESH = pl.DeviceIdType.MESH
F32, BF16 = jnp.float32, jnp.bfloat16


def ratio(num, den):
    return jnp.where(den == 0.0, 0.0, num / jnp.where(den == 0.0, 1.0, den))


def coefficients(moments):
    zero = jnp.zeros_like(moments[0])
    rho = [zero + 1.0] + [zero] * ITERS
    delta = [zero + 1.0] + [zero] * (ITERS - 1)
    xi = [zero] * ITERS
    gamma = moments[0]
    for k in range(ITERS):
        across = [(delta[i] if i < ITERS else zero) - (delta[i - 1] if i else zero) for i in range(k + 2)]
        curve = sum(delta[i] * across[j] * moments[i + j] for i in range(k + 1) for j in range(k + 2))
        alpha = ratio(gamma, curve)
        for i in range(k + 1):
            xi[i] = xi[i] + alpha * delta[i]
        for i in range(k + 2):
            rho[i] = rho[i] - alpha * across[i]
        if k + 1 < ITERS:
            later = sum(rho[i] * rho[j] * moments[i + j] for i in range(k + 2) for j in range(k + 2))
            beta = ratio(later, gamma)
            for i in range(k + 2):
                delta[i] = rho[i] + beta * delta[i]
            gamma = later
    return xi, rho


def halves(value):
    high = value.astype(BF16)
    low = (value - high.astype(F32)).astype(BF16)
    return jnp.concatenate([high, low], axis=1)


def times(left, right):
    stacked = jnp.concatenate([piece for piece in right for _ in range(2)], axis=0)
    wide = jnp.dot(left, stacked, preferred_element_type=F32)
    half = wide.shape[1] // 2
    return wide[:, :half] + wide[:, half:]


def kernel(
    nx, ny, paired,
    volt, source, cap, diag, inverse, east, south, mask,
    volt_out, res_out,
    U, T, X, L, PC, STE, ETE, HN, HD, HE, HW, PD, PE, RB, MOM, MR, G,
    load_sem, sN, rN, sD, rD, sR, rE, sP, rW, sB, rB, sG, rG,
):
    _, R, C, B, S = U.shape
    ix, iy = lax.axis_index("gx"), lax.axis_index("gy")
    north, south_on = ix > 0, ix < nx - 1
    west, east_on = iy > 0, iy < ny - 1

    loads = [
        pltpu.make_async_copy(src, dst, load_sem.at[n])
        for n, (src, dst) in enumerate(
            [(volt, U.at[0]), (south, T.at[2]), (east, T.at[1]), (inverse, T.at[3]), (diag, T.at[4]), (source, T.at[0])]
        )
    ]
    for load in loads:
        load.start()

    barrier = pltpu.get_barrier_semaphore()
    for d in range(1, nx):
        pl.semaphore_signal(barrier, inc=1, device_id={"gx": lax.rem(ix + d, nx)}, device_id_type=MESH)
    for d in range(1, ny):
        pl.semaphore_signal(barrier, inc=1, device_id={"gy": lax.rem(iy + d, ny)}, device_id_type=MESH)
    pl.semaphore_wait(barrier, nx + ny - 2)

    odd, nz = lax.rem(ix, 2) == 1, nx // 2
    AHEAD = min(3, C)
    EARLY = C - C // 4

    def place(c):
        return lax.rem(c + C - 1, C)

    def column(j):
        return lax.rem(j + 1, C)

    def long_south(z, c):
        return place(c) * nz < C * (nz - 1 - z)

    if paired:
        even = jnp.logical_not(odd)
        detour_south = lambda c: odd & long_south(lax.div(ix - 1, 2), c)
        detour_north = lambda c: even & jnp.logical_not(long_south(lax.div(ix, 2) - 1, c))
        passes_south = lambda c: even & (ix < nx - 2) & long_south(lax.div(ix, 2), c)
        passes_north = lambda c: odd & (ix > 2) & jnp.logical_not(long_south(lax.div(ix - 3, 2), c))

    def raw_north(k, c, far=False):
        src = volt.at[0, c] if k == 0 else U.at[k, 0, c]
        dst, sem, hop = (RB, rB, -1) if far else (HN, rN, 1)
        return pltpu.make_async_remote_copy(src, dst.at[k, c], sN.at[k, c], sem.at[k, c], device_id={"gx": ix - hop}, device_id_type=MESH)

    def product_south(k, c, far=False):
        dst, sem, hop = (RB, rB, -1) if far else (HD, rD, 1)
        return pltpu.make_async_remote_copy(PD.at[k, c], dst.at[k, c], sD.at[k, c], sem.at[k, c], device_id={"gx": ix + hop}, device_id_type=MESH)

    def start_raw(k, c):
        if not paired:
            raw_north(k, c).start()
            return
        far = detour_north(c)

        @pl.when(far)
        def _():
            raw_north(k, c, True).start()

        @pl.when(jnp.logical_not(far))
        def _():
            raw_north(k, c).start()

    def start_product(k, c):
        if not paired:
            product_south(k, c).start()
            return
        far = detour_south(c)

        @pl.when(far)
        def _():
            product_south(k, c, True).start()

        @pl.when(jnp.logical_not(far))
        def _():
            product_south(k, c).start()

    def onward(k, c, south):
        dst, sem, hop = (HD, rD, 2) if south else (HN, rN, -2)
        return pltpu.make_async_remote_copy(RB.at[k, c], dst.at[k, c], sB.at[k, c], sem.at[k, c], device_id={"gx": ix + hop}, device_id_type=MESH)

    def arrived(k, c):
        return pltpu.make_async_remote_copy(RB.at[k, c], RB.at[k, c], sB.at[k, c], rB.at[k, c], device_id={"gx": ix - 1}, device_id_type=MESH)

    def pass_south(k, c):
        if paired:
            @pl.when(passes_south(c))
            def _():
                arrived(k, c).wait_recv()
                onward(k, c, True).start()

    def pass_north(k, c):
        if paired:
            @pl.when(passes_north(c))
            def _():
                arrived(k, c).wait_recv()
                onward(k, c, False).start()

    def raw_west(k, r):
        src = volt.at[r, 0] if k == 0 else U.at[k, r, 0]
        return pltpu.make_async_remote_copy(src, HE.at[k, r], sR.at[k, r], rE.at[k, r], device_id={"gy": iy - 1}, device_id_type=MESH)

    def product_east(k, r):
        return pltpu.make_async_remote_copy(PE.at[k, r], HW.at[k, r], sP.at[k, r], rW.at[k, r], device_id={"gy": iy + 1}, device_id_type=MESH)

    @pl.when(north)
    def _():
        @pl.loop(0, AHEAD)
        def _(j):
            start_raw(0, column(j))

    @pl.when(west)
    def _():
        @pl.loop(0, R)
        def _(r):
            raw_west(0, r).start()

    def send_south(k, c):
        @pl.when(south_on)
        def _():
            PD[k, c] = times(STE[c], [X[k % 2, R, c + 1]])
            start_product(k, c)

    def send_side(k, r):
        @pl.when(east_on)
        def _():
            PE[k, r] = times(ETE[r], [X[k % 2, r + 1, C]])
            product_east(k, r).start()

        if k:
            @pl.when(west)
            def _():
                raw_west(k, r).start()

    MOM[...] = jnp.zeros_like(MOM)
    blank = jnp.zeros((B, 2 * S), BF16)
    for parity in range(2):
        for r in range(R + 2):
            X[parity, r, 0] = blank
            X[parity, r, C + 1] = blank
        for c in range(C + 2):
            X[parity, 0, c] = blank
            X[parity, R + 1, c] = blank
    for r in range(R):
        L[r, 0, :, 2 * B:4 * B] = blank
    for c in range(C):
        L[0, c, :, 6 * B:8 * B] = blank

    loads[0].wait()
    loads[1].wait()

    @pl.loop(0, C)
    def _(j):
        c = column(j)
        X[0, R, c + 1] = halves(U[0, R - 1, c])
        live = T[2, R - 1, c] * mask[R - 1, 1, c].astype(F32)
        STE[c] = halves(live.T)
        send_south(0, c)

        @pl.when(north & (j < C - AHEAD))
        def _():
            start_raw(0, column(j + AHEAD))

    loads[2].wait()

    @pl.loop(0, R)
    def _(r):
        X[0, r + 1, C] = halves(U[0, r, C - 1])
        live = T[1, r, C - 1] * mask[r, 0, C - 1].astype(F32)
        ETE[r] = halves(live.T)
        send_side(0, r)

    loads[3].wait()

    @pl.loop(0, R * C)
    def _(n):
        r, c = n // C, n % C

        X[0, r + 1, c + 1] = halves(U[0, r, c])
        PC[r, c] = halves(T[3, r, c])
        e_live = T[1, r, c] * mask[r, 0, c].astype(F32)
        L[r, c, :, 0:2 * B] = halves(e_live)
        s_live = T[2, r, c] * mask[r, 1, c].astype(F32)
        L[r, c, :, 4 * B:6 * B] = halves(s_live)

        @pl.when(c < C - 1)
        def _():
            L[r, c + 1, :, 2 * B:4 * B] = halves(e_live.T)

        @pl.when(r < R - 1)
        def _():
            L[r + 1, c, :, 6 * B:8 * B] = halves(s_live.T)

    loads[4].wait()
    loads[5].wait()

    def gather(m, former, latter):
        MOM[m] += jnp.sum((former * latter).reshape(B // 8, 8, S), axis=0)

    def image(k, r, c, extra=None):
        p = k % 2
        t = times(L[r, c], [X[p, r + 1, c + 2], X[p, r + 1, c], X[p, r + 2, c + 1], X[p, r, c + 1]])
        if extra is not None:
            for part in extra:
                t = t + part
        if k == 0:
            charge = jnp.broadcast_to(cap[r, pl.ds(c, 1), :], (S, B)).T
            t = t + (T[0, r, c] + charge * U[0, r, c]) - times(halves(T[4, r, c]), [X[0, r + 1, c + 1]])
        return t

    def finish(k, r, c, t):
        T[k, r, c] = t
        if k:
            gather(2 * k - 1, U[k, r, c], t)
        if k < ITERS:
            split = halves(t)
            u = times(PC[r, c], [split])
            U[k + 1, r, c] = u
            X[(k + 1) % 2, r + 1, c + 1] = halves(u)
            gather(2 * k, u, t)

    inner = list(range(1, R - 1))
    edges = [0] if R == 1 else [0, R - 1]
    def side_waits(k, rows):
        p = k % 2

        @pl.when(east_on)
        def _():
            for r in rows:
                raw_west(k, r).wait_recv()
                X[p, r + 1, C + 1] = halves(HE[k, r])

        @pl.when(west)
        def _():
            for r in rows:
                product_east(k, r).wait_recv()

        @pl.when(jnp.logical_not(west))
        def _():
            for r in rows:
                HW[k, r] = jnp.zeros((B, S), F32)

    def edge(k, c, side):
        p = k % 2

        if k < ITERS:
            @pl.when(south_on)
            def _():
                raw_north(k, c).wait_recv()
                X[p, R + 1, c + 1] = halves(HN[k, c])
        else:
            X[p, R + 1, c + 1] = blank

        @pl.when(north)
        def _():
            product_south(k, c).wait_recv()

        @pl.when(jnp.logical_not(north))
        def _():
            HD[k, c] = jnp.zeros((B, S), F32)

        first = (c == 0).astype(F32)
        ts = [
            image(k, r, c, ([first * HW[k, r]] if side else []) + ([HD[k, c]] if r == 0 else []))
            for r in edges
        ]
        for r, t in zip(edges, ts):
            finish(k, r, c, t)
        if k < ITERS:
            if k + 1 < ITERS:
                @pl.when(north)
                def _():
                    start_raw(k + 1, c)

            send_south(k + 1, c)
        else:
            gather(2 * k - 1, U[k, 0, c], HD[k, c])

    def passes(k, first, last):
        @pl.loop(first, last)
        def _(j):
            pass_south(k, column(j))
            if k < ITERS:
                pass_north(k, column(j))

    soon = (C // 4, C // 2)
    for k in range(STEPS):
        if k == 0:
            passes(k, 0, soon[0])

        @pl.loop(1, C - 1)
        def _(c):
            ts = [image(k, r, c) for r in inner]
            for r, t in zip(inner, ts):
                finish(k, r, c, t)

        if k == 0:
            passes(k, soon[0], soon[1])

        side_waits(k, inner)
        ts = [image(k, r, C - 1) for r in inner] + [image(k, r, 0, [HW[k, r]]) for r in inner]
        for n, t in enumerate(ts):
            r, c = (inner[n], C - 1) if n < len(inner) else (inner[n - len(inner)], 0)
            finish(k, r, c, t)
        if k < ITERS:
            for r in inner:
                send_side(k + 1, r)

        def passing(j):
            @pl.when(j >= (soon[1] if k == 0 else 0))
            def _():
                pass_south(k, column(j))
                if k < ITERS:
                    pass_north(k, column(j))

        @pl.loop(0, C - 2)
        def _(j):
            edge(k, column(j), False)
            passing(j)

        side_waits(k, edges)

        @pl.loop(C - 2, C)
        def _(j):
            edge(k, column(j), True)
            passing(j)

        if k < ITERS:
            for r in edges:
                send_side(k + 1, r)
        if k + 1 == ITERS:
            @pl.when(north)
            def _():
                @pl.loop(0, EARLY)
                def _(j):
                    start_raw(ITERS, column(j))

    def sent(k):
        @pl.loop(0, C)
        def _(c):
            @pl.when(north)
            def _():
                raw_north(k, c).wait_send()

            @pl.when(south_on)
            def _():
                product_south(k, c).wait_send()

            if paired:
                @pl.when(passes_south(c) | passes_north(c))
                def _():
                    onward(k, c, True).wait_send()

        @pl.loop(0, R)
        def _(r):
            @pl.when(west)
            def _():
                raw_west(k, r).wait_send()

            @pl.when(east_on)
            def _():
                product_east(k, r).wait_send()

    MR[0] = jnp.sum(MOM[...], axis=1)
    base = 0
    for stage, (axis, size, me) in enumerate((("gy", ny, iy), ("gx", nx, ix))):
        copies = []
        for d in range(1, size):
            copies.append(pltpu.make_async_remote_copy(
                MR.at[stage], G.at[base + me], sG.at[base + d], rG.at[base + d],
                device_id={axis: lax.rem(me + d, size)}, device_id_type=MESH))
        for copy in copies:
            copy.start()
        if stage:
            @pl.when(north)
            def _():
                @pl.loop(EARLY, C)
                def _(j):
                    start_raw(ITERS, column(j))

            @pl.loop(0, EARLY)
            def _(j):
                pass_north(ITERS, column(j))

            for k in range(ITERS):
                sent(k)
        G[base + me] = MR[stage]
        for copy in copies:
            copy.wait()
        total = G[base]
        for d in range(1, size):
            total = total + G[base + d]
        MR[stage + 1] = total
        base += size

    @pl.loop(EARLY, C)
    def _(j):
        pass_north(ITERS, column(j))

    summed = MR[2]
    xi, rho = coefficients([summed[m:m + 1] for m in range(2 * ITERS)])

    for r in range(R):
        @pl.loop(0, C)
        def _(c):
            v = U[0, r, c]
            for i in range(ITERS):
                v = v + xi[i] * U[i + 1, r, c]
            volt_out[r, c] = v
            w = rho[0] * T[0, r, c]
            for i in range(1, STEPS):
                w = w + rho[i] * T[i, r, c]
            res_out[r, c] = w

    @pl.when(south_on)
    def _():
        @pl.loop(0, C)
        def _(j):
            c = column(j)
            raw_north(ITERS, c).wait_recv()
            late = times(L[R - 1, c, :, 4 * B:6 * B], [halves(HN[ITERS, c])])
            res_out[R - 1, c] = res_out[R - 1, c] + rho[ITERS] * late

    sent(ITERS)


def shards(nx, ny, paired, volt, source, cap, diag, inverse, east, south, mask):
    R, C, B, S = volt.shape
    mask = jnp.swapaxes(mask, 1, 2)
    hbm = pl.BlockSpec(memory_space=pl.ANY)
    vmem = pl.BlockSpec(memory_space=pltpu.VMEM)
    smem = pl.BlockSpec(memory_space=pltpu.SMEM)
    dma = pltpu.SemaphoreType.DMA
    shape = pltpu.VMEM(volt.shape, F32)
    return pl.pallas_call(
        functools.partial(kernel, nx, ny, paired),
        out_shape=(shape, shape),
        in_specs=[hbm, hbm, vmem, hbm, hbm, hbm, hbm, smem],
        out_specs=(vmem, vmem),
        scratch_shapes=[
            pltpu.VMEM((STEPS, R, C, B, S), F32),
            pltpu.VMEM((STEPS, R, C, B, S), F32),
            pltpu.VMEM((2, R + 2, C + 2, B, 2 * S), BF16),
            pltpu.VMEM((R, C, B, 8 * B), BF16),
            pltpu.VMEM((R, C, B, 2 * B), BF16),
            pltpu.VMEM((C, B, 2 * B), BF16),
            pltpu.VMEM((R, B, 2 * B), BF16),
            pltpu.VMEM((STEPS, C, B, S), F32),
            pltpu.VMEM((STEPS, C, B, S), F32),
            pltpu.VMEM((STEPS, R, B, S), F32),
            pltpu.VMEM((STEPS, R, B, S), F32),
            pltpu.VMEM((STEPS, C, B, S), F32),
            pltpu.VMEM((STEPS, R, B, S), F32),
            pltpu.VMEM((STEPS, C, B, S), F32),
            pltpu.VMEM((2 * ITERS, 8, S), F32),
            pltpu.VMEM((3, 2 * ITERS, S), F32),
            pltpu.VMEM((nx + ny, 2 * ITERS, S), F32),
            dma((6,)),
            dma((STEPS, C)), dma((STEPS, C)),
            dma((STEPS, C)), dma((STEPS, C)),
            dma((STEPS, R)), dma((STEPS, R)),
            dma((STEPS, R)), dma((STEPS, R)),
            dma((STEPS, C)), dma((STEPS, C)),
            dma((nx + ny,)), dma((nx + ny,)),
        ],
        compiler_params=pltpu.CompilerParams(
            collective_id=0, has_side_effects=True, vmem_limit_bytes=58 * 1024 * 1024
        ),
    )(volt, source, cap, diag, inverse, east, south, mask)


def two_rows(mesh):
    places = [getattr(d, "coords", None) for d in mesh.devices[:, 0]]
    if None in places or len(places) % 2 or len(places) < 4:
        return False
    hops = [sum(abs(int(p) - int(q)) for p, q in zip(a, b)) for a, b in zip(places, places[1:])]
    return all(hop == 1 + i % 2 for i, hop in enumerate(hops))


def solution(mesh):
    grid = P("gx", "gy", None, None)
    in_specs = (grid, grid, P("gx", "gy", None), grid, grid, grid, grid, P("gx", "gy", None))
    body = functools.partial(shards, mesh.shape["gx"], mesh.shape["gy"], two_rows(mesh))
    return jax.shard_map(body, mesh=mesh, in_specs=in_specs, out_specs=(grid, grid), check_vma=False)
```

```python
import functools

import jax
import jax.numpy as jnp
from jax import lax
from jax.experimental import pallas as pl
from jax.experimental.pallas import tpu as pltpu
from jax.sharding import PartitionSpec as P

ITERS = 4
STEPS = ITERS + 1
MESH = pl.DeviceIdType.MESH
F32, BF16 = jnp.float32, jnp.bfloat16


def ratio(num, den):
    return jnp.where(den == 0.0, 0.0, num / jnp.where(den == 0.0, 1.0, den))


def before_last(moments):
    zero = jnp.zeros_like(moments[0])
    rho = [zero + 1.0] + [zero] * ITERS
    delta = [zero + 1.0] + [zero] * (ITERS - 1)
    xi = [zero] * ITERS
    gamma = moments[0]
    for k in range(ITERS):
        across = [(delta[i] if i < ITERS else zero) - (delta[i - 1] if i else zero) for i in range(k + 2)]
        curve = sum(
            delta[i] * across[j] * moments[i + j]
            for i in range(k + 1) for j in range(k + 2) if i + j < len(moments)
        )
        if k + 1 == ITERS:
            return xi, delta, rho, across, gamma, curve
        alpha = ratio(gamma, curve)
        for i in range(k + 1):
            xi[i] = xi[i] + alpha * delta[i]
        for i in range(k + 2):
            rho[i] = rho[i] - alpha * across[i]
        later = sum(rho[i] * rho[j] * moments[i + j] for i in range(k + 2) for j in range(k + 2))
        beta = ratio(later, gamma)
        for i in range(k + 2):
            delta[i] = rho[i] + beta * delta[i]
        gamma = later


def halves(value):
    high = value.astype(BF16)
    low = (value - high.astype(F32)).astype(BF16)
    return jnp.concatenate([high, low], axis=1)


def times(left, right):
    stacked = jnp.concatenate([piece for piece in right for _ in range(2)], axis=0)
    wide = jnp.dot(left, stacked, preferred_element_type=F32)
    half = wide.shape[1] // 2
    return wide[:, :half] + wide[:, half:]


def kernel(
    nx, ny, paired,
    volt, source, cap, diag, inverse, east, south, mask,
    volt_out, dir_out, res_out, img_out, step_out,
    U, T, X, L, PC, STE, ETE, HN, HD, HE, HW, PD, PE, RB, MOM, G, F,
    load_sem, sN, rN, sD, rD, sR, rE, sP, rW, sB, rB, sG, sF, here,
):
    _, R, C, B, S = U.shape
    ix, iy = lax.axis_index("gx"), lax.axis_index("gy")
    north, south_on = ix > 0, ix < nx - 1
    west, east_on = iy > 0, iy < ny - 1

    loads = [
        pltpu.make_async_copy(src, dst, load_sem.at[n])
        for n, (src, dst) in enumerate(
            [(volt, U.at[0]), (south, T.at[2]), (east, T.at[1]), (inverse, T.at[3]), (diag, T.at[4]), (source, T.at[0])]
        )
    ]
    for load in loads:
        load.start()

    barrier = pltpu.get_barrier_semaphore()
    for d in range(1, nx):
        pl.semaphore_signal(barrier, inc=1, device_id={"gx": lax.rem(ix + d, nx)}, device_id_type=MESH)
    for d in range(1, ny):
        pl.semaphore_signal(barrier, inc=1, device_id={"gy": lax.rem(iy + d, ny)}, device_id_type=MESH)
    pl.semaphore_wait(barrier, nx + ny - 2)
    for d in range(1, ny):
        pl.semaphore_signal(here, inc=1, device_id={"gy": lax.rem(iy + d, ny)}, device_id_type=MESH)

    odd, nz = lax.rem(ix, 2) == 1, nx // 2
    AHEAD = min(3, C)
    EARLY = C - C // 4
    HOLD = C // 2

    def place(c):
        return lax.rem(c + C - 1, C)

    def column(j):
        return lax.rem(j + 1, C)

    def long_south(z, c):
        return place(c) * nz < C * (nz - 1 - z)

    if paired:
        even = jnp.logical_not(odd)
        detour_south = lambda c: odd & long_south(lax.div(ix - 1, 2), c)
        detour_north = lambda c: even & jnp.logical_not(long_south(lax.div(ix, 2) - 1, c))
        passes_south = lambda c: even & (ix < nx - 2) & long_south(lax.div(ix, 2), c)
        passes_north = lambda c: odd & (ix > 2) & jnp.logical_not(long_south(lax.div(ix - 3, 2), c))

    def raw_north(k, c, far=False):
        src = volt.at[0, c] if k == 0 else U.at[k, 0, c]
        dst, sem, hop = (RB, rB, -1) if far else (HN, rN, 1)
        return pltpu.make_async_remote_copy(src, dst.at[k, c], sN, sem.at[k % 2, c], device_id={"gx": ix - hop}, device_id_type=MESH)

    def product_south(k, c, far=False):
        dst, sem, hop = (RB, rB, -1) if far else (HD, rD, 1)
        return pltpu.make_async_remote_copy(PD.at[k, c], dst.at[k, c], sD, sem.at[k % 2, c], device_id={"gx": ix + hop}, device_id_type=MESH)

    def start_raw(k, c, own=True, through=True):
        if not paired:
            if own:
                raw_north(k, c).start()
            return
        far = detour_north(c)
        if own:
            @pl.when(north & far)
            def _():
                raw_north(k, c, True).start()

            @pl.when(north & odd)
            def _():
                raw_north(k, c).start()
        if through:
            @pl.when(north & even & jnp.logical_not(far))
            def _():
                raw_north(k, c).start()

    def start_product(k, c, own=True, through=True):
        if not paired:
            if own:
                product_south(k, c).start()
            return
        far = detour_south(c)
        if own:
            @pl.when(far)
            def _():
                product_south(k, c, True).start()

            @pl.when(even)
            def _():
                product_south(k, c).start()
        if through:
            @pl.when(odd & jnp.logical_not(far))
            def _():
                product_south(k, c).start()

    def start_through(k, c):
        if paired:
            if k < ITERS:
                start_raw(k, c, own=False)
            if k:
                @pl.when(south_on)
                def _():
                    start_product(k, c, own=False)

    def onward(k, c, south):
        dst, sem, hop = (HD, rD, 2) if south else (HN, rN, -2)
        return pltpu.make_async_remote_copy(RB.at[k, c], dst.at[k, c], sB.at[k], sem.at[k % 2, c], device_id={"gx": ix + hop}, device_id_type=MESH)

    def arrived(k, c):
        return pltpu.make_async_remote_copy(RB.at[k, c], RB.at[k, c], sB.at[k], rB.at[k % 2, c], device_id={"gx": ix - 1}, device_id_type=MESH)

    def pass_south(k, c):
        if paired:
            @pl.when(passes_south(c))
            def _():
                arrived(k, c).wait_recv()
                onward(k, c, True).start()

    def pass_north(k, c):
        if paired:
            @pl.when(passes_north(c))
            def _():
                arrived(k, c).wait_recv()
                onward(k, c, False).start()

    def raw_west(k, r):
        src = volt.at[r, 0] if k == 0 else U.at[k, r, 0]
        return pltpu.make_async_remote_copy(src, HE.at[k, r], sR, rE.at[k % 2, r], device_id={"gy": iy - 1}, device_id_type=MESH)

    def product_east(k, r):
        return pltpu.make_async_remote_copy(PE.at[k, r], HW.at[k, r], sP, rW.at[k % 2, r], device_id={"gy": iy + 1}, device_id_type=MESH)

    @pl.when(north)
    def _():
        @pl.loop(0, AHEAD)
        def _(j):
            start_raw(0, column(j))

    @pl.when(west)
    def _():
        @pl.loop(0, R)
        def _(r):
            raw_west(0, r).start()

    def send_south(k, c):
        @pl.when(south_on)
        def _():
            PD[k, c] = times(STE[c], [X[k % 2, R, c + 1]])
            start_product(k, c, through=k == 0)

    def send_side(k, r):
        @pl.when(east_on)
        def _():
            PE[k, r] = times(ETE[r], [X[k % 2, r + 1, C]])
            product_east(k, r).start()

        if k:
            @pl.when(west)
            def _():
                raw_west(k, r).start()

    MOM[...] = jnp.zeros_like(MOM)
    blank = jnp.zeros((B, 2 * S), BF16)
    for parity in range(2):
        for r in range(R + 2):
            X[parity, r, 0] = blank
            X[parity, r, C + 1] = blank
        for c in range(C + 2):
            X[parity, 0, c] = blank
            X[parity, R + 1, c] = blank
    for r in range(R):
        L[r, 0, :, 2 * B:4 * B] = blank
    for c in range(C):
        L[0, c, :, 6 * B:8 * B] = blank

    loads[0].wait()
    loads[1].wait()

    @pl.loop(0, C)
    def _(j):
        c = column(j)
        X[0, R, c + 1] = halves(U[0, R - 1, c])
        live = T[2, R - 1, c] * mask[R - 1, 1, c].astype(F32)
        STE[c] = halves(live.T)
        send_south(0, c)

        @pl.when(north & (j < C - AHEAD))
        def _():
            start_raw(0, column(j + AHEAD))

    loads[2].wait()

    @pl.loop(0, R)
    def _(r):
        X[0, r + 1, C] = halves(U[0, r, C - 1])
        live = T[1, r, C - 1] * mask[r, 0, C - 1].astype(F32)
        ETE[r] = halves(live.T)
        send_side(0, r)

    loads[3].wait()

    @pl.loop(0, R * C)
    def _(n):
        r, c = n // C, n % C

        X[0, r + 1, c + 1] = halves(U[0, r, c])
        PC[r, c] = halves(T[3, r, c])
        e_live = T[1, r, c] * mask[r, 0, c].astype(F32)
        L[r, c, :, 0:2 * B] = halves(e_live)
        s_live = T[2, r, c] * mask[r, 1, c].astype(F32)
        L[r, c, :, 4 * B:6 * B] = halves(s_live)

        @pl.when(c < C - 1)
        def _():
            L[r, c + 1, :, 2 * B:4 * B] = halves(e_live.T)

        @pl.when(r < R - 1)
        def _():
            L[r + 1, c, :, 6 * B:8 * B] = halves(s_live.T)

    loads[4].wait()
    loads[5].wait()

    def gather(m, former, latter):
        MOM[m] += jnp.sum((former * latter).reshape(B // 8, 8, S), axis=0)

    def image(k, r, c, extra=None):
        p = k % 2
        t = times(L[r, c], [X[p, r + 1, c + 2], X[p, r + 1, c], X[p, r + 2, c + 1], X[p, r, c + 1]])
        if extra is not None:
            for part in extra:
                t = t + part
        if k == 0:
            charge = jnp.broadcast_to(cap[r, pl.ds(c, 1), :], (S, B)).T
            t = t + (T[0, r, c] + charge * U[0, r, c]) - times(halves(T[4, r, c]), [X[0, r + 1, c + 1]])
        return t

    def finish(k, r, c, t):
        T[k, r, c] = t
        if k:
            gather(2 * k - 1, U[k, r, c], t)
        if k < ITERS:
            split = halves(t)
            u = times(PC[r, c], [split])
            U[k + 1, r, c] = u
            X[(k + 1) % 2, r + 1, c + 1] = halves(u)
            gather(2 * k, u, t)

    inner = list(range(1, R - 1))
    edges = [0] if R == 1 else [0, R - 1]
    def side_waits(k, rows):
        p = k % 2

        @pl.when(east_on)
        def _():
            for r in rows:
                raw_west(k, r).wait_recv()
                X[p, r + 1, C + 1] = halves(HE[k, r])

        @pl.when(west)
        def _():
            for r in rows:
                product_east(k, r).wait_recv()

        @pl.when(jnp.logical_not(west))
        def _():
            for r in rows:
                HW[k, r] = jnp.zeros((B, S), F32)

    def edge(k, c, side):
        p = k % 2

        if k < ITERS:
            @pl.when(south_on)
            def _():
                raw_north(k, c).wait_recv()
                X[p, R + 1, c + 1] = halves(HN[k, c])
        else:
            X[p, R + 1, c + 1] = blank

        @pl.when(north)
        def _():
            product_south(k, c).wait_recv()

        @pl.when(jnp.logical_not(north))
        def _():
            HD[k, c] = jnp.zeros((B, S), F32)

        first = (c == 0).astype(F32)
        ts = [
            image(k, r, c, ([first * HW[k, r]] if side else []) + ([HD[k, c]] if r == 0 else []))
            for r in edges
        ]
        for r, t in zip(edges, ts):
            finish(k, r, c, t)
        if k < ITERS:
            raws = k + 1 < ITERS
            if raws:
                @pl.when(north & jnp.logical_not(odd))
                def _():
                    start_raw(k + 1, c, through=False)

            send_south(k + 1, c)
            if raws:
                @pl.when(north & odd)
                def _():
                    start_raw(k + 1, c, through=False)
        else:
            gather(2 * k - 1, U[k, 0, c], HD[k, c])

    me, count = ix * ny + iy, nx * ny

    def spread(ref, sems):
        @pl.loop(1, count)
        def _(d):
            other = lax.rem(me + d, count)
            pltpu.make_async_remote_copy(
                ref.at[me], ref.at[me], sems.at[0], sems.at[1],
                device_id={"gx": lax.div(other, ny), "gy": lax.rem(other, ny)}, device_id_type=MESH).start()

    def spreading(ref, sems):
        others = ref.at[pl.ds(0, count - 1)]
        return pltpu.make_async_remote_copy(others, others, sems.at[0], sems.at[1], device_id={"gx": ix}, device_id_type=MESH)

    def now(j):
        return (j < EARLY) | jnp.logical_not(odd) if paired else j < EARLY

    def pass_on(k, c):
        pass_south(k, c)
        if k < ITERS:
            pass_north(k, c)

    for k in range(STEPS):
        if k == 0:
            @pl.loop(0, C // 4)
            def _(j):
                pass_on(k, column(j))

        @pl.loop(1, C - 1)
        def _(c):
            ts = [image(k, r, c) for r in inner]
            for r, t in zip(inner, ts):
                finish(k, r, c, t)

        if k == 0:
            @pl.loop(C // 4, C // 2)
            def _(j):
                pass_on(k, column(j))

        side_waits(k, inner)
        ts = [image(k, r, C - 1) for r in inner] + [image(k, r, 0, [HW[k, r]]) for r in inner]
        for n, t in enumerate(ts):
            r, c = (inner[n], C - 1) if n < len(inner) else (inner[n - len(inner)], 0)
            finish(k, r, c, t)
        if k < ITERS:
            for r in inner:
                send_side(k + 1, r)

        if k == ITERS:
            @pl.when(north)
            def _():
                @pl.loop(0, C)
                def _(j):
                    @pl.when(now(j))
                    def _():
                        start_raw(ITERS, column(j), through=False)
        elif k:
            @pl.loop(C - HOLD, C)
            def _(j):
                start_through(k, column(j))

        lead = C // 2 if k == 0 else 0

        def held(j):
            @pl.when(j >= HOLD)
            def _():
                if k < ITERS:
                    start_through(k + 1, column(j - HOLD))
                elif paired:
                    start_raw(k, column(j - HOLD), own=False)

        @pl.loop(0, C - 2)
        def _(j):
            @pl.when(j + lead < C)
            def _():
                pass_on(k, column(j + lead))

            edge(k, column(j), False)
            held(j)

        side_waits(k, edges)

        @pl.loop(C - 2, C)
        def _(j):
            if not lead:
                pass_on(k, column(j))
            edge(k, column(j), True)
            held(j)

        if k < ITERS:
            for r in edges:
                send_side(k + 1, r)
        if k + 1 == ITERS:
            pl.semaphore_wait(here, ny - 1)
            @pl.loop(C - HOLD, C)
            def _(j):
                start_through(ITERS, column(j))

            G[me] = jnp.sum(MOM[...], axis=1)
            spread(G, sG)

    F[me] = jnp.sum(MOM[2 * ITERS - 1], axis=0, keepdims=True)
    spread(F, sF)

    @pl.when(north)
    def _():
        @pl.loop(EARLY, C)
        def _(j):
            @pl.when(jnp.logical_not(now(j)))
            def _():
                start_raw(ITERS, column(j), through=False)

        if paired:
            @pl.loop(C - HOLD, C)
            def _(j):
                start_raw(ITERS, column(j), own=False)

    @pl.loop(0, C // 2)
    def _(j):
        pass_north(ITERS, column(j))

    spreading(G, sG).wait_recv()
    summed = jnp.sum(G[...], axis=0)
    xi, delta, rho, across, gamma, curve = before_last([summed[m:m + 1] for m in range(2 * ITERS - 1)])

    def mix(weights, terms):
        total = None
        for weight, term in zip(weights, terms):
            total = weight * term if total is None else total + weight * term
        return total

    for r in range(R):
        @pl.loop(0, C)
        def _(c):
            us = [U[i + 1, r, c] for i in range(ITERS)]
            ts = [T[i, r, c] for i in range(STEPS)]
            volt_out[r, c] = U[0, r, c] + mix(xi[:ITERS - 1], us)
            dir_out[r, c] = mix(delta, us)
            res_out[r, c] = mix(rho[:ITERS], ts)
            img_out[r, c] = mix(across, ts)

        rest = C - C // 2

        @pl.loop(C - rest + rest * r // R, C - rest + rest * (r + 1) // R)
        def _(j):
            pass_north(ITERS, column(j))

    @pl.when(south_on)
    def _():
        @pl.loop(0, C)
        def _(j):
            c = column(j)
            raw_north(ITERS, c).wait_recv()
            late = times(L[R - 1, c, :, 4 * B:6 * B], [halves(HN[ITERS, c])])
            img_out[R - 1, c] = img_out[R - 1, c] + across[ITERS] * late

    spreading(F, sF).wait_recv()
    last = jnp.sum(F[...], axis=0)
    step_out[...] = ratio(gamma, curve + delta[ITERS - 1] * across[ITERS] * last)
    spreading(G, sG).wait_send()
    spreading(F, sF).wait_send()

    def sent(cond, ref, sem):
        @pl.when(cond)
        def _():
            pltpu.make_async_remote_copy(ref, ref, sem, sem, device_id={"gx": ix}, device_id_type=MESH).wait_send()

    sent(north, HN, sN)
    sent(south_on, PD, sD)
    sent(west, HE, sR)
    sent(east_on, PE, sP)
    if paired:
        for z in range(nz - 1):
            souths = -(-C * (nz - 1 - z) // nz)
            for k in range(STEPS):
                if souths:
                    sent(ix == 2 * z, RB.at[k, pl.ds(0, souths)], sB.at[k])
                if C - souths:
                    sent(ix == 2 * z + 3, RB.at[k, pl.ds(0, C - souths)], sB.at[k])


def shards(nx, ny, paired, volt, source, cap, diag, inverse, east, south, mask):
    R, C, B, S = volt.shape
    mask = jnp.swapaxes(mask, 1, 2)
    hbm = pl.BlockSpec(memory_space=pl.ANY)
    vmem = pl.BlockSpec(memory_space=pltpu.VMEM)
    smem = pl.BlockSpec(memory_space=pltpu.SMEM)
    dma = pltpu.SemaphoreType.DMA
    shape = pltpu.VMEM(volt.shape, F32)
    volt, direction, res, image, step = pl.pallas_call(
        functools.partial(kernel, nx, ny, paired),
        out_shape=(shape, shape, shape, shape, pltpu.VMEM((1, S), F32)),
        in_specs=[hbm, hbm, vmem, hbm, hbm, hbm, hbm, smem],
        out_specs=(vmem,) * 5,
        scratch_shapes=[
            pltpu.VMEM((STEPS, R, C, B, S), F32),
            pltpu.VMEM((STEPS, R, C, B, S), F32),
            pltpu.VMEM((2, R + 2, C + 2, B, 2 * S), BF16),
            pltpu.VMEM((R, C, B, 8 * B), BF16),
            pltpu.VMEM((R, C, B, 2 * B), BF16),
            pltpu.VMEM((C, B, 2 * B), BF16),
            pltpu.VMEM((R, B, 2 * B), BF16),
            pltpu.VMEM((STEPS, C, B, S), F32),
            pltpu.VMEM((STEPS, C, B, S), F32),
            pltpu.VMEM((STEPS, R, B, S), F32),
            pltpu.VMEM((STEPS, R, B, S), F32),
            pltpu.VMEM((STEPS, C, B, S), F32),
            pltpu.VMEM((STEPS, R, B, S), F32),
            pltpu.VMEM((STEPS, C, B, S), F32),
            pltpu.VMEM((2 * ITERS, 8, S), F32),
            pltpu.VMEM((nx * ny, 2 * ITERS, S), F32),
            pltpu.VMEM((nx * ny, 1, S), F32),
            dma((6,)),
            dma, dma((2, C)),
            dma, dma((2, C)),
            dma, dma((2, R)),
            dma, dma((2, R)),
            dma((STEPS,)), dma((2, C)),
            dma((2,)), dma((2,)), pltpu.SemaphoreType.REGULAR,
        ],
        compiler_params=pltpu.CompilerParams(
            collective_id=0, has_side_effects=True, vmem_limit_bytes=55 * 1024 * 1024
        ),
    )(volt, source, cap, diag, inverse, east, south, mask)
    return volt + step * direction, res - step * image


def two_rows(mesh):
    places = [getattr(d, "coords", None) for d in mesh.devices[:, 0]]
    if None in places or len(places) % 2 or len(places) < 4:
        return False
    hops = [sum(abs(int(p) - int(q)) for p, q in zip(a, b)) for a, b in zip(places, places[1:])]
    return all(hop == 1 + i % 2 for i, hop in enumerate(hops))


def solution(mesh):
    grid = P("gx", "gy", None, None)
    in_specs = (grid, grid, P("gx", "gy", None), grid, grid, grid, grid, P("gx", "gy", None))
    body = functools.partial(shards, mesh.shape["gx"], mesh.shape["gy"], two_rows(mesh))
    return jax.shard_map(body, mesh=mesh, in_specs=in_specs, out_specs=(grid, grid), check_vma=False)
```

```python
import functools

import jax
import jax.numpy as jnp
from jax import lax
from jax.experimental import pallas as pl
from jax.experimental.pallas import tpu as pltpu
from jax.sharding import PartitionSpec as P

ITERS = 4
STEPS = ITERS + 1
MESH = pl.DeviceIdType.MESH
F32, BF16 = jnp.float32, jnp.bfloat16


def ratio(num, den):
    return jnp.where(den == 0.0, 0.0, num / jnp.where(den == 0.0, 1.0, den))


def before_last(moments):
    zero = jnp.zeros_like(moments[0])
    rho = [zero + 1.0] + [zero] * ITERS
    delta = [zero + 1.0] + [zero] * (ITERS - 1)
    xi = [zero] * ITERS
    gamma = moments[0]
    for k in range(ITERS):
        across = [(delta[i] if i < ITERS else zero) - (delta[i - 1] if i else zero) for i in range(k + 2)]
        curve = sum(
            delta[i] * across[j] * moments[i + j]
            for i in range(k + 1) for j in range(k + 2) if i + j < len(moments)
        )
        if k + 1 == ITERS:
            return xi, delta, rho, across, gamma, curve
        alpha = ratio(gamma, curve)
        for i in range(k + 1):
            xi[i] = xi[i] + alpha * delta[i]
        for i in range(k + 2):
            rho[i] = rho[i] - alpha * across[i]
        later = sum(rho[i] * rho[j] * moments[i + j] for i in range(k + 2) for j in range(k + 2))
        beta = ratio(later, gamma)
        for i in range(k + 2):
            delta[i] = rho[i] + beta * delta[i]
        gamma = later


def halves(value):
    high = value.astype(BF16)
    low = (value - high.astype(F32)).astype(BF16)
    return jnp.concatenate([high, low], axis=1)


def times(left, right):
    stacked = jnp.concatenate([piece for piece in right for _ in range(2)], axis=0)
    wide = jnp.dot(left, stacked, preferred_element_type=F32)
    half = wide.shape[1] // 2
    return wide[:, :half] + wide[:, half:]


def kernel(
    nx, ny, paired,
    volt, source, cap_in, diag, inverse, east, south, mask_in,
    volt_out, dir_out, res_out, img_out, step_out,
    U, T, X, L, PC, STE, ETE, HN, HD, HE, HW, PD, PE, RB, MOM, G, F, cap, mask,
    load_sem, sN, rN, sD, rD, sR, rE, sP, rW, sB, rB, sG, sF, here,
):
    _, R, C, B, S = U.shape
    ix, iy = lax.axis_index("gx"), lax.axis_index("gy")
    north, south_on = ix > 0, ix < nx - 1
    west, east_on = iy > 0, iy < ny - 1

    loads = [
        pltpu.make_async_copy(src, dst, load_sem.at[n])
        for n, (src, dst) in enumerate(
            [(volt, U.at[0]), (south, T.at[2]), (east, T.at[1]), (inverse, T.at[3]), (diag, T.at[4]), (source, T.at[0]), (cap_in, cap), (mask_in, mask)]
        )
    ]
    for load in loads:
        load.start()

    barrier = pltpu.get_barrier_semaphore()
    for d in range(1, nx):
        pl.semaphore_signal(barrier, inc=1, device_id={"gx": lax.rem(ix + d, nx)}, device_id_type=MESH)
    for d in range(1, ny):
        pl.semaphore_signal(barrier, inc=1, device_id={"gy": lax.rem(iy + d, ny)}, device_id_type=MESH)
    pl.semaphore_wait(barrier, nx + ny - 2)
    for d in range(1, ny):
        pl.semaphore_signal(here, inc=1, device_id={"gy": lax.rem(iy + d, ny)}, device_id_type=MESH)

    odd, nz = lax.rem(ix, 2) == 1, nx // 2
    AHEAD = min(3, C)
    TAIL = min(2, C - AHEAD)
    EARLY = C - C // 4
    HOLD = C // 2

    def place(c):
        return lax.rem(c + C - 1, C)

    def column(j):
        return lax.rem(j + 1, C)

    def long_south(z, c):
        return place(c) * nz < C * (nz - 1 - z)

    if paired:
        even = jnp.logical_not(odd)
        detour_south = lambda c: odd & long_south(lax.div(ix - 1, 2), c)
        detour_north = lambda c: even & jnp.logical_not(long_south(lax.div(ix, 2) - 1, c))
        passes_south = lambda c: even & (ix < nx - 2) & long_south(lax.div(ix, 2), c)
        passes_north = lambda c: odd & (ix > 2) & jnp.logical_not(long_south(lax.div(ix - 3, 2), c))

    def raw_north(k, c, far=False):
        src = volt.at[0, c] if k == 0 else U.at[k, 0, c]
        dst, sem, hop = (RB, rB, -1) if far else (HN, rN, 1)
        return pltpu.make_async_remote_copy(src, dst.at[k, c], sN, sem.at[k % 2, c], device_id={"gx": ix - hop}, device_id_type=MESH)

    def product_south(k, c, far=False):
        dst, sem, hop = (RB, rB, -1) if far else (HD, rD, 1)
        return pltpu.make_async_remote_copy(PD.at[k, c], dst.at[k, c], sD, sem.at[k % 2, c], device_id={"gx": ix + hop}, device_id_type=MESH)

    def start_raw(k, c, own=True, through=True):
        if not paired:
            if own:
                raw_north(k, c).start()
            return
        far = detour_north(c)
        if own:
            @pl.when(north & far)
            def _():
                raw_north(k, c, True).start()

            @pl.when(north & odd)
            def _():
                raw_north(k, c).start()
        if through:
            @pl.when(north & even & jnp.logical_not(far))
            def _():
                raw_north(k, c).start()

    def start_product(k, c, own=True, through=True):
        if not paired:
            if own:
                product_south(k, c).start()
            return
        far = detour_south(c)
        if own:
            @pl.when(far)
            def _():
                product_south(k, c, True).start()

            @pl.when(even)
            def _():
                product_south(k, c).start()
        if through:
            @pl.when(odd & jnp.logical_not(far))
            def _():
                product_south(k, c).start()

    def start_through(k, c):
        if paired:
            if k < ITERS:
                start_raw(k, c, own=False)
            if k:
                @pl.when(south_on)
                def _():
                    start_product(k, c, own=False)

    def onward(k, c, south):
        dst, sem, hop = (HD, rD, 2) if south else (HN, rN, -2)
        return pltpu.make_async_remote_copy(RB.at[k, c], dst.at[k, c], sB.at[k], sem.at[k % 2, c], device_id={"gx": ix + hop}, device_id_type=MESH)

    def arrived(k, c):
        return pltpu.make_async_remote_copy(RB.at[k, c], RB.at[k, c], sB.at[k], rB.at[k % 2, c], device_id={"gx": ix - 1}, device_id_type=MESH)

    def pass_south(k, c):
        if paired:
            @pl.when(passes_south(c))
            def _():
                arrived(k, c).wait_recv()
                onward(k, c, True).start()

    def pass_north(k, c):
        if paired:
            @pl.when(passes_north(c))
            def _():
                arrived(k, c).wait_recv()
                onward(k, c, False).start()

    def raw_west(k, r):
        src = volt.at[r, 0] if k == 0 else U.at[k, r, 0]
        return pltpu.make_async_remote_copy(src, HE.at[k, r], sR, rE.at[k % 2, r], device_id={"gy": iy - 1}, device_id_type=MESH)

    def product_east(k, r):
        return pltpu.make_async_remote_copy(PE.at[k, r], HW.at[k, r], sP, rW.at[k % 2, r], device_id={"gy": iy + 1}, device_id_type=MESH)

    @pl.when(north)
    def _():
        @pl.loop(0, AHEAD)
        def _(j):
            start_raw(0, column(j))

        if paired:
            @pl.loop(C - TAIL, C)
            def _(j):
                @pl.when(even)
                def _():
                    start_raw(0, column(j))

    @pl.when(west)
    def _():
        @pl.loop(0, R)
        def _(r):
            raw_west(0, r).start()

    def send_south(k, c):
        @pl.when(south_on)
        def _():
            PD[k, c] = times(STE[c], [X[k % 2, R, c + 1]])
            start_product(k, c, through=k == 0)

    def send_side(k, r):
        @pl.when(east_on)
        def _():
            PE[k, r] = times(ETE[r], [X[k % 2, r + 1, C]])
            product_east(k, r).start()

        if k:
            @pl.when(west)
            def _():
                raw_west(k, r).start()

    MOM[...] = jnp.zeros_like(MOM)
    blank = jnp.zeros((B, 2 * S), BF16)
    for parity in range(2):
        for r in range(R + 2):
            X[parity, r, 0] = blank
            X[parity, r, C + 1] = blank
        for c in range(C + 2):
            X[parity, 0, c] = blank
            X[parity, R + 1, c] = blank
    for r in range(R):
        L[r, 0, :, 2 * B:4 * B] = blank
    for c in range(C):
        L[0, c, :, 6 * B:8 * B] = blank

    loads[7].wait()
    loads[0].wait()
    loads[1].wait()

    @pl.loop(0, C)
    def _(j):
        c = column(j)
        X[0, R, c + 1] = halves(U[0, R - 1, c])
        live = T[2, R - 1, c] * mask[R - 1, 1, c].astype(F32)
        STE[c] = halves(live.T)
        send_south(0, c)

        gone = even & (j + AHEAD >= C - TAIL) if paired else False

        @pl.when(north & (j < C - AHEAD) & jnp.logical_not(gone))
        def _():
            start_raw(0, column(j + AHEAD))

    loads[2].wait()

    @pl.loop(0, R)
    def _(r):
        X[0, r + 1, C] = halves(U[0, r, C - 1])
        live = T[1, r, C - 1] * mask[r, 0, C - 1].astype(F32)
        ETE[r] = halves(live.T)
        send_side(0, r)

    loads[3].wait()

    @pl.loop(0, R * C)
    def _(n):
        r, c = n // C, n % C

        X[0, r + 1, c + 1] = halves(U[0, r, c])
        PC[r, c] = halves(T[3, r, c])
        e_live = T[1, r, c] * mask[r, 0, c].astype(F32)
        L[r, c, :, 0:2 * B] = halves(e_live)
        s_live = T[2, r, c] * mask[r, 1, c].astype(F32)
        L[r, c, :, 4 * B:6 * B] = halves(s_live)

        @pl.when(c < C - 1)
        def _():
            L[r, c + 1, :, 2 * B:4 * B] = halves(e_live.T)

        @pl.when(r < R - 1)
        def _():
            L[r + 1, c, :, 6 * B:8 * B] = halves(s_live.T)

    loads[4].wait()
    loads[5].wait()
    loads[6].wait()

    def gather(m, former, latter):
        MOM[m] += jnp.sum((former * latter).reshape(B // 8, 8, S), axis=0)

    def image(k, r, c, extra=None):
        p = k % 2
        t = times(L[r, c], [X[p, r + 1, c + 2], X[p, r + 1, c], X[p, r + 2, c + 1], X[p, r, c + 1]])
        if extra is not None:
            for part in extra:
                t = t + part
        if k == 0:
            charge = jnp.broadcast_to(cap[r, pl.ds(c, 1), :], (S, B)).T
            t = t + (T[0, r, c] + charge * U[0, r, c]) - times(halves(T[4, r, c]), [X[0, r + 1, c + 1]])
        return t

    def finish(k, r, c, t):
        T[k, r, c] = t
        if k:
            gather(2 * k - 1, U[k, r, c], t)
        if k < ITERS:
            split = halves(t)
            u = times(PC[r, c], [split])
            U[k + 1, r, c] = u
            X[(k + 1) % 2, r + 1, c + 1] = halves(u)
            gather(2 * k, u, t)

    inner = list(range(1, R - 1))
    edges = [0] if R == 1 else [0, R - 1]
    def side_waits(k, rows):
        p = k % 2

        @pl.when(east_on)
        def _():
            for r in rows:
                raw_west(k, r).wait_recv()
                X[p, r + 1, C + 1] = halves(HE[k, r])

        @pl.when(west)
        def _():
            for r in rows:
                product_east(k, r).wait_recv()

        @pl.when(jnp.logical_not(west))
        def _():
            for r in rows:
                HW[k, r] = jnp.zeros((B, S), F32)

    def edge(k, c, side):
        p = k % 2

        if k < ITERS:
            @pl.when(south_on)
            def _():
                raw_north(k, c).wait_recv()
                X[p, R + 1, c + 1] = halves(HN[k, c])
        else:
            X[p, R + 1, c + 1] = blank

        @pl.when(north)
        def _():
            product_south(k, c).wait_recv()

        @pl.when(jnp.logical_not(north))
        def _():
            HD[k, c] = jnp.zeros((B, S), F32)

        first = (c == 0).astype(F32)
        ts = [
            image(k, r, c, ([first * HW[k, r]] if side else []) + ([HD[k, c]] if r == 0 else []))
            for r in edges
        ]
        for r, t in zip(edges, ts):
            finish(k, r, c, t)
        if k < ITERS:
            raws = k + 1 < ITERS
            if raws:
                @pl.when(north & jnp.logical_not(odd))
                def _():
                    start_raw(k + 1, c, through=False)

            send_south(k + 1, c)
            if raws:
                @pl.when(north & odd)
                def _():
                    start_raw(k + 1, c, through=False)
        else:
            gather(2 * k - 1, U[k, 0, c], HD[k, c])

    me, count = ix * ny + iy, nx * ny

    def spread(ref, sems):
        @pl.loop(1, count)
        def _(d):
            other = lax.rem(me + d, count)
            pltpu.make_async_remote_copy(
                ref.at[me], ref.at[me], sems.at[0], sems.at[1],
                device_id={"gx": lax.div(other, ny), "gy": lax.rem(other, ny)}, device_id_type=MESH).start()

    def spreading(ref, sems):
        others = ref.at[pl.ds(0, count - 1)]
        return pltpu.make_async_remote_copy(others, others, sems.at[0], sems.at[1], device_id={"gx": ix}, device_id_type=MESH)

    def now(j):
        return (j < EARLY) | jnp.logical_not(odd) if paired else j < EARLY

    def pass_on(k, c):
        pass_south(k, c)
        if k < ITERS:
            pass_north(k, c)

    for k in range(STEPS):
        if k == 0:
            @pl.loop(0, C // 4)
            def _(j):
                pass_on(k, column(j))

        @pl.loop(1, C - 1)
        def _(c):
            ts = [image(k, r, c) for r in inner]
            for r, t in zip(inner, ts):
                finish(k, r, c, t)

        if k == 0:
            @pl.loop(C // 4, C // 2)
            def _(j):
                pass_on(k, column(j))

        side_waits(k, inner)
        ts = [image(k, r, C - 1) for r in inner] + [image(k, r, 0, [HW[k, r]]) for r in inner]
        for n, t in enumerate(ts):
            r, c = (inner[n], C - 1) if n < len(inner) else (inner[n - len(inner)], 0)
            finish(k, r, c, t)
        if k < ITERS:
            for r in inner:
                send_side(k + 1, r)

        if 0 < k < ITERS:
            @pl.loop(C - HOLD, C)
            def _(j):
                start_through(k, column(j))

        lead = C // 2 if k == 0 else 0

        def held(j):
            @pl.when(j >= HOLD)
            def _():
                if k < ITERS:
                    start_through(k + 1, column(j - HOLD))
                elif paired:
                    @pl.when(ix < 4)
                    def _():
                        start_raw(k, column(j - HOLD), own=False)

        @pl.loop(0, C - 2)
        def _(j):
            @pl.when(j + lead < C)
            def _():
                pass_on(k, column(j + lead))

            edge(k, column(j), False)
            held(j)

        side_waits(k, edges)

        @pl.loop(C - 2, C)
        def _(j):
            if not lead:
                pass_on(k, column(j))
            edge(k, column(j), True)
            held(j)

        if k < ITERS:
            for r in edges:
                send_side(k + 1, r)
        if k + 1 == ITERS:
            pl.semaphore_wait(here, ny - 1)
            @pl.loop(C - HOLD, C)
            def _(j):
                start_through(ITERS, column(j))

            G[me] = jnp.sum(MOM[...], axis=1)
            spread(G, sG)

            @pl.when(north)
            def _():
                @pl.loop(0, C)
                def _(j):
                    @pl.when(now(j))
                    def _():
                        start_raw(ITERS, column(j), through=False)

    F[me] = jnp.sum(MOM[2 * ITERS - 1], axis=0, keepdims=True)
    spread(F, sF)

    @pl.when(north)
    def _():
        @pl.loop(EARLY, C)
        def _(j):
            @pl.when(jnp.logical_not(now(j)))
            def _():
                start_raw(ITERS, column(j), through=False)

        if paired:
            @pl.loop(0, C)
            def _(j):
                @pl.when((ix >= 4) | (j >= C - HOLD))
                def _():
                    start_raw(ITERS, column(j), own=False)

    @pl.loop(0, C // 2)
    def _(j):
        pass_north(ITERS, column(j))

    spreading(G, sG).wait_recv()
    summed = jnp.sum(G[...], axis=0)
    xi, delta, rho, across, gamma, curve = before_last([summed[m:m + 1] for m in range(2 * ITERS - 1)])

    def mix(weights, terms):
        total = None
        for weight, term in zip(weights, terms):
            total = weight * term if total is None else total + weight * term
        return total

    for r in range(R):
        @pl.loop(0, C)
        def _(c):
            us = [U[i + 1, r, c] for i in range(ITERS)]
            ts = [T[i, r, c] for i in range(STEPS)]
            volt_out[r, c] = U[0, r, c] + mix(xi[:ITERS - 1], us)
            dir_out[r, c] = mix(delta, us)
            res_out[r, c] = mix(rho[:ITERS], ts)
            img_out[r, c] = mix(across, ts)

        rest = C - C // 2

        @pl.loop(C - rest + rest * r // R, C - rest + rest * (r + 1) // R)
        def _(j):
            pass_north(ITERS, column(j))

    @pl.when(south_on)
    def _():
        @pl.loop(0, C)
        def _(j):
            c = column(j)
            raw_north(ITERS, c).wait_recv()
            late = times(L[R - 1, c, :, 4 * B:6 * B], [halves(HN[ITERS, c])])
            img_out[R - 1, c] = img_out[R - 1, c] + across[ITERS] * late

    spreading(F, sF).wait_recv()
    last = jnp.sum(F[...], axis=0)
    step_out[...] = ratio(gamma, curve + delta[ITERS - 1] * across[ITERS] * last)
    spreading(G, sG).wait_send()
    spreading(F, sF).wait_send()

    def sent(cond, ref, sem):
        @pl.when(cond)
        def _():
            pltpu.make_async_remote_copy(ref, ref, sem, sem, device_id={"gx": ix}, device_id_type=MESH).wait_send()

    sent(north, HN, sN)
    sent(south_on, PD, sD)
    sent(west, HE, sR)
    sent(east_on, PE, sP)
    if paired:
        for z in range(nz - 1):
            souths = -(-C * (nz - 1 - z) // nz)
            for k in range(STEPS):
                if souths:
                    sent(ix == 2 * z, RB.at[k, pl.ds(0, souths)], sB.at[k])
                if C - souths:
                    sent(ix == 2 * z + 3, RB.at[k, pl.ds(0, C - souths)], sB.at[k])


def shards(nx, ny, paired, volt, source, cap, diag, inverse, east, south, mask):
    R, C, B, S = volt.shape
    mask = jnp.swapaxes(mask, 1, 2)
    hbm = pl.BlockSpec(memory_space=pl.ANY)
    vmem = pl.BlockSpec(memory_space=pltpu.VMEM)
    dma = pltpu.SemaphoreType.DMA
    shape = pltpu.VMEM(volt.shape, F32)
    volt, direction, res, image, step = pl.pallas_call(
        functools.partial(kernel, nx, ny, paired),
        out_shape=(shape, shape, shape, shape, pltpu.VMEM((1, S), F32)),
        in_specs=[hbm] * 8,
        out_specs=(vmem,) * 5,
        scratch_shapes=[
            pltpu.VMEM((STEPS, R, C, B, S), F32),
            pltpu.VMEM((STEPS, R, C, B, S), F32),
            pltpu.VMEM((2, R + 2, C + 2, B, 2 * S), BF16),
            pltpu.VMEM((R, C, B, 8 * B), BF16),
            pltpu.VMEM((R, C, B, 2 * B), BF16),
            pltpu.VMEM((C, B, 2 * B), BF16),
            pltpu.VMEM((R, B, 2 * B), BF16),
            pltpu.VMEM((STEPS, C, B, S), F32),
            pltpu.VMEM((STEPS, C, B, S), F32),
            pltpu.VMEM((STEPS, R, B, S), F32),
            pltpu.VMEM((STEPS, R, B, S), F32),
            pltpu.VMEM((STEPS, C, B, S), F32),
            pltpu.VMEM((STEPS, R, B, S), F32),
            pltpu.VMEM((STEPS, C, B, S), F32),
            pltpu.VMEM((2 * ITERS, 8, S), F32),
            pltpu.VMEM((nx * ny, 2 * ITERS, S), F32),
            pltpu.VMEM((nx * ny, 1, S), F32),
            pltpu.VMEM((R, C, B), F32),
            pltpu.SMEM((R, 2, C), jnp.int32),
            dma((8,)),
            dma, dma((2, C)),
            dma, dma((2, C)),
            dma, dma((2, R)),
            dma, dma((2, R)),
            dma((STEPS,)), dma((2, C)),
            dma((2,)), dma((2,)), pltpu.SemaphoreType.REGULAR,
        ],
        compiler_params=pltpu.CompilerParams(
            collective_id=0, has_side_effects=True, vmem_limit_bytes=55 * 1024 * 1024
        ),
    )(volt, source, cap, diag, inverse, east, south, mask)
    return volt + step * direction, res - step * image


def two_rows(mesh):
    places = [getattr(d, "coords", None) for d in mesh.devices[:, 0]]
    if None in places or len(places) % 2 or len(places) < 4:
        return False
    hops = [sum(abs(int(p) - int(q)) for p, q in zip(a, b)) for a, b in zip(places, places[1:])]
    return all(hop == 1 + i % 2 for i, hop in enumerate(hops))


def solution(mesh):
    grid = P("gx", "gy", None, None)
    in_specs = (grid, grid, P("gx", "gy", None), grid, grid, grid, grid, P("gx", "gy", None))
    body = functools.partial(shards, mesh.shape["gx"], mesh.shape["gy"], two_rows(mesh))
    return jax.shard_map(body, mesh=mesh, in_specs=in_specs, out_specs=(grid, grid), check_vma=False)
```
